32 devices in a mesh: groups: 2 (over y), dp: 4 (over z), mp: 4 (over x, core).
Axes of the slice: x: 2, y: 2, z: 4, core: 2. Of those that a mesh axis runs over, the one named last changes fastest.
Arguments:
- tokens: bfloat16 [1024, 7168], P(('groups', 'dp')), parts along dimension 0, may hold values from -20 to 20, as said below
- w_down: bfloat16 [7168, 1536], P('dp', 'mp'), may hold values from -3 to 3, as said below
- gain: float32 [1536], P('mp'), may hold values from 0.25 to 1.75
- w_up: bfloat16 [1536, 26112], P('dp', 'mp'), may hold values from -0.15625 to 0.15625
- head_counts: int32 [4], replicated, may hold values from 30 to 34, as said below
- cotangent: bfloat16 [1024, 26112], P(('groups', 'dp'), 'mp'), parts along dimension 0, may hold values from -6 to 6
Outputs:
- queries: bfloat16 [1024, 26112], P(('groups', 'dp'), 'mp'), parts along dimension 0
- grad_tokens: bfloat16 [1024, 7168], P(('groups', 'dp'), 'mp'), parts along dimension 0
The draws below stay inside these ranges and needn't reach their ends.
There are 2 independent parts, one for each index of `groups`. The reference program is written for one: setup_inputs(seed, part) draws one part's arguments, and reference() takes and returns one part's arrays. A program takes and returns all parts, laid end to end along the dimension named above; an argument that names none is the same for every part. Nothing has to cross between parts.
Inputs may be any that keep to these rules, and one draw needn't show every extreme that they name: `tokens`: hidden states of order one with token scales that differ. `w_down`: entries of order 7168^(-1/2). `head_counts`: the entries sum to 128; one of them is 34.
All inputs are finite; a program needn't handle non-finite values.
Results may differ from the reference program's by a relative error of at most 0.018.
Values may be sent and summed in bfloat16 or wider, within the bound.
A program may use at most 128 MiB of HBM per device.

```python
import math
import jax
import jax.numpy as jnp
from jax import lax

D = 7168
LAT = 1536
HEADS = 128
HD = 192
HSLOT = 34
TOKENS = 512
COLS = 26112
N_MP = 4


def draw_tokens(key, part):
    base_key, scale_key = jax.random.split(key, 2)
    values = jnp.clip(jax.random.normal(base_key, (TOKENS, D), jnp.float32), -6.0, 6.0)
    scales = jnp.exp(jax.random.uniform(scale_key, (TOKENS, 1), jnp.float32, math.log(0.3), math.log(3.0)))
    return (values * scales).astype(jnp.bfloat16)


def draw_w_down(key, part):
    base_key, scale_key = jax.random.split(key, 2)
    values = jax.random.normal(base_key, (D, LAT), jnp.float32)
    values = jnp.clip(values, -6.0, 6.0)
    rising = 0.55 + 1.1 * jnp.arange(LAT, dtype=jnp.float32) / LAT
    col_scale = jnp.exp(jax.random.uniform(scale_key, (1, LAT), jnp.float32, -0.7, 0.7)) * rising
    return (values * col_scale * D ** (-0.5)).astype(jnp.bfloat16)


def draw_head_counts(key, part):
    order_key, extra_key = jax.random.split(jax.random.fold_in(key, 11))
    rank_of = jax.random.permutation(order_key, N_MP).astype(jnp.int32)
    excess = HSLOT - HEADS // N_MP
    extra = jax.random.randint(extra_key, (), 0, excess + 1).astype(jnp.int32)
    delta = jnp.where(rank_of == 0, excess, jnp.where(rank_of == 1, -excess, jnp.where(rank_of == 2, extra, jnp.where(rank_of == 3, -extra, 0))))
    return (HEADS // N_MP + delta).astype(jnp.int32)


def shard_levels(stream_key, extent, shards, smallest, top_value):
    def one(axis_at, blocks):
        steps = jax.random.uniform(jax.random.fold_in(jax.random.fold_in(stream_key, 6), axis_at), (blocks,), jnp.float32, smallest / len(shards), top_value / len(shards))
        return jnp.repeat(jnp.exp(steps), extent[axis_at] // blocks).reshape((-1,) + (1,) * (len(extent) - axis_at - 1))

    level = one(*shards[0])
    for cut in shards[1:]:
        level = level * one(*cut)
    return level


def gaussian(own_key, dims, deviation, most, cuts=(), held_as=jnp.bfloat16):
    array = jax.random.normal(own_key, dims, jnp.float32) * deviation
    if len(cuts) > 0:
        array = shard_levels(own_key, dims, cuts, -0.22, 0.18) * array
    return jnp.clip(array, min=-most, max=most).astype(held_as)


def setup_inputs(seed: int = 0, part: int = 0) -> dict:
    keys = jax.random.split(jax.random.key(seed), 7)
    part_keys = jax.random.split(jax.random.fold_in(keys[6], part), 7)
    return {
        "tokens": draw_tokens(jax.random.fold_in(jax.random.fold_in(keys[6], part), 71), part),
        "w_down": draw_w_down(jax.random.fold_in(keys[6], 71), part),
        "gain": jnp.clip(1.0 + 0.15 * jax.random.normal(keys[2], (LAT,), jnp.float32), 0.25, 1.75),
        "w_up": gaussian(keys[3], (LAT, COLS), LAT ** -0.5, 0.15625, ((0, 4), (1, 4))),
        "head_counts": draw_head_counts(jax.random.fold_in(keys[6], 71), part),
        "cotangent": gaussian(part_keys[5], (TOKENS, COLS), 1.0, 6.0, ((0, 4), (1, 4))),
    }


def reference(tokens, w_down, gain, w_up, head_counts, cotangent):
    latent_raw = jnp.dot(tokens, w_down, preferred_element_type=jnp.float32)
    root_mean = jnp.sqrt(lax.optimization_barrier(jnp.mean(latent_raw * latent_raw, axis=1, keepdims=True)) + 1e-06)
    latent = (latent_raw / root_mean * gain).astype(jnp.bfloat16)
    block_cols = HSLOT * HD
    column = jnp.arange(N_MP * block_cols, dtype=jnp.int32)
    owner = column // block_cols
    slot_index = column % block_cols // HD
    keep_mask = (slot_index < head_counts[owner]).astype(jnp.float32)
    queries = (jnp.dot(latent, w_up, preferred_element_type=jnp.float32) * keep_mask).astype(jnp.bfloat16)
    masked = cotangent * keep_mask.astype(jnp.bfloat16)
    grad_latent = lax.dot_general(masked, w_up, (((1,), (1,)), ((), ())), preferred_element_type=jnp.float32)
    inner_dot = lax.optimization_barrier(jnp.sum(gain * grad_latent * latent_raw, axis=1, keepdims=True))
    grad_raw = (gain * grad_latent / root_mean - latent_raw * inner_dot / (LAT * root_mean ** 3)).astype(jnp.bfloat16)
    width = LAT // N_MP
    running = jnp.zeros((tokens.shape[0], D), jnp.float32)
    for block in range(N_MP):
        product = lax.dot_general(grad_raw[:, block * width:(block + 1) * width], w_down[:, block * width:(block + 1) * width], (((1,), (1,)), ((), ())), preferred_element_type=jnp.float32)
        running = running + lax.optimization_barrier(product.astype(jnp.bfloat16)).astype(jnp.float32)
    return (queries, running.astype(jnp.bfloat16))
```

```python
import jax
import jax.numpy as jnp
from jax import lax
from jax.sharding import PartitionSpec as P

HD = 192


def contract_last(left, right):
    return lax.dot_general(
        left, right, (((1,), (1,)), ((), ())), preferred_element_type=jnp.float32
    )


def keep_mask_of(head_counts, block_cols):
    position = lax.axis_index("mp")
    held_heads = lax.dynamic_slice_in_dim(head_counts, position, 1, 0)
    slot_index = jnp.arange(block_cols, dtype=jnp.int32) // HD
    return (slot_index < held_heads).astype(jnp.float32)


def gather_weights_body(tokens, w_down, gain, w_up, head_counts, cotangent):
    latent_width = w_down.shape[1] * lax.axis_size("mp")
    keep_mask = keep_mask_of(head_counts, w_up.shape[1])
    down_whole = lax.all_gather(w_down, "dp", axis=0, tiled=True)
    latent_raw = jnp.dot(tokens, down_whole, preferred_element_type=jnp.float32)
    squares = lax.psum(jnp.sum(latent_raw * latent_raw, axis=1, keepdims=True), "mp")
    root_mean = jnp.sqrt(squares / latent_width + 1e-06)
    latent_local = (latent_raw / root_mean * gain).astype(jnp.bfloat16)
    latent = lax.all_gather(latent_local, "mp", axis=1, tiled=True)
    masked = cotangent * keep_mask.astype(jnp.bfloat16)
    up_whole = lax.all_gather(w_up, "dp", axis=0, tiled=True)
    query_total = jnp.dot(latent, up_whole, preferred_element_type=jnp.float32)
    grad_partial = contract_last(masked, up_whole)
    queries = (query_total * keep_mask).astype(jnp.bfloat16)
    grad_latent = lax.psum_scatter(
        grad_partial.astype(jnp.bfloat16), "mp", scatter_dimension=1, tiled=True
    ).astype(jnp.float32)
    inner_dot = lax.psum(jnp.sum(gain * grad_latent * latent_raw, axis=1, keepdims=True), "mp")
    grad_raw = (
        gain * grad_latent / root_mean - latent_raw * inner_dot / (latent_width * root_mean**3)
    ).astype(jnp.bfloat16)
    partial_value = contract_last(grad_raw, down_whole).astype(jnp.bfloat16)
    grad_tokens = lax.psum_scatter(partial_value, "mp", scatter_dimension=1, tiled=True)
    return (queries, grad_tokens)


def move_tokens_body(tokens, w_down, gain, w_up, head_counts, cotangent):
    n = lax.axis_size("mp")
    swap = [(i * n + j, j * n + i) for i in range(n) for j in range(n)]
    position = lax.axis_index("mp")
    latent_width = w_down.shape[1] * n
    keep_mask = keep_mask_of(head_counts, w_up.shape[1])

    def transpose_owner(block):
        return lax.ppermute(block, ("dp", "mp"), swap)

    rows = w_down.shape[0]
    tokens_block = lax.dynamic_slice_in_dim(tokens, position * rows, rows, 1)
    tokens_cols = lax.all_gather(transpose_owner(tokens_block), "mp", axis=0, tiled=True)
    raw_partial = jnp.dot(tokens_cols, w_down, preferred_element_type=jnp.float32)
    latent_raw = lax.psum_scatter(raw_partial, "dp", scatter_dimension=0, tiled=True)
    squares = lax.psum(jnp.sum(latent_raw * latent_raw, axis=1, keepdims=True), "mp")
    root_mean = jnp.sqrt(squares / latent_width + 1e-06)
    latent_local = (latent_raw / root_mean * gain).astype(jnp.bfloat16)
    latent = lax.all_gather(transpose_owner(latent_local), "mp", axis=0, tiled=True)
    query_partial = (
        jnp.dot(latent, w_up, preferred_element_type=jnp.float32) * keep_mask
    ).astype(jnp.bfloat16)
    masked = cotangent * keep_mask.astype(jnp.bfloat16)
    masked_all = lax.all_gather(masked, "dp", axis=0, tiled=True)
    queries = lax.psum_scatter(query_partial, "dp", scatter_dimension=0, tiled=True)
    grad_partial = contract_last(masked_all, w_up).astype(jnp.bfloat16)
    grad_latent = transpose_owner(
        lax.psum_scatter(grad_partial, "mp", scatter_dimension=0, tiled=True)
    ).astype(jnp.float32)
    inner_dot = lax.psum(jnp.sum(gain * grad_latent * latent_raw, axis=1, keepdims=True), "mp")
    grad_raw = (
        gain * grad_latent / root_mean - latent_raw * inner_dot / (latent_width * root_mean**3)
    ).astype(jnp.bfloat16)
    grad_raw_all = lax.all_gather(grad_raw, "dp", axis=0, tiled=True)
    token_partial = contract_last(grad_raw_all, w_down).astype(jnp.bfloat16)
    grad_tokens = transpose_owner(
        lax.psum_scatter(token_partial, "mp", scatter_dimension=0, tiled=True)
    )
    return (queries, grad_tokens)


def solution(mesh):
    in_specs = (
        P(("groups", "dp"), None),
        P("dp", "mp"),
        P("mp"),
        P("dp", "mp"),
        P(),
        P(("groups", "dp"), "mp"),
    )
    out_specs = (P(("groups", "dp"), "mp"), P(("groups", "dp"), "mp"))
    square = mesh.shape["dp"] == mesh.shape["mp"]
    body = move_tokens_body if square else gather_weights_body
    return jax.shard_map(body, mesh=mesh, in_specs=in_specs, out_specs=out_specs, check_vma=False)
```

```python
import functools

import jax
import jax.numpy as jnp
from jax import lax
from jax.experimental import pallas as pl
from jax.experimental.pallas import tpu as pltpu
from jax.sharding import PartitionSpec as P

HD = 192
MESH = pl.DeviceIdType.MESH


def contract_last(left, right):
    return lax.dot_general(
        left, right, (((1,), (1,)), ((), ())), preferred_element_type=jnp.float32
    )


def keep_mask_of(head_counts, block_cols):
    position = lax.axis_index("mp")
    held_heads = lax.dynamic_slice_in_dim(head_counts, position, 1, 0)
    slot_index = jnp.arange(block_cols, dtype=jnp.int32) // HD
    return (slot_index < held_heads).astype(jnp.float32)


def gather_weights_body(tokens, w_down, gain, w_up, head_counts, cotangent):
    latent_width = w_down.shape[1] * lax.axis_size("mp")
    keep_mask = keep_mask_of(head_counts, w_up.shape[1])
    down_whole = lax.all_gather(w_down, "dp", axis=0, tiled=True)
    latent_raw = jnp.dot(tokens, down_whole, preferred_element_type=jnp.float32)
    squares = lax.psum(jnp.sum(latent_raw * latent_raw, axis=1, keepdims=True), "mp")
    root_mean = jnp.sqrt(squares / latent_width + 1e-06)
    latent_local = (latent_raw / root_mean * gain).astype(jnp.bfloat16)
    latent = lax.all_gather(latent_local, "mp", axis=1, tiled=True)
    masked = cotangent * keep_mask.astype(jnp.bfloat16)
    up_whole = lax.all_gather(w_up, "dp", axis=0, tiled=True)
    query_total = jnp.dot(latent, up_whole, preferred_element_type=jnp.float32)
    grad_partial = contract_last(masked, up_whole)
    queries = (query_total * keep_mask).astype(jnp.bfloat16)
    grad_latent = lax.psum_scatter(
        grad_partial.astype(jnp.bfloat16), "mp", scatter_dimension=1, tiled=True
    ).astype(jnp.float32)
    inner_dot = lax.psum(jnp.sum(gain * grad_latent * latent_raw, axis=1, keepdims=True), "mp")
    grad_raw = (
        gain * grad_latent / root_mean - latent_raw * inner_dot / (latent_width * root_mean**3)
    ).astype(jnp.bfloat16)
    partial_value = contract_last(grad_raw, down_whole).astype(jnp.bfloat16)
    grad_tokens = lax.psum_scatter(partial_value, "mp", scatter_dimension=1, tiled=True)
    return (queries, grad_tokens)


def exchange_kernel(
    n, chunks, tile, latent_ref, w_ref, keep_ref, cot_ref, queries_ref, grad_ref,
    masked_w, parts, landed, total, send_sem, recv_sem,
):
    me = lax.axis_index("dp")
    count, cols = cot_ref.shape
    rows = count // chunks

    barrier = pltpu.get_barrier_semaphore()
    for step in (1, n - 1):
        pl.semaphore_signal(
            barrier, inc=1, device_id={"dp": lax.rem(me + step, n)}, device_id_type=MESH
        )
    pl.semaphore_wait(barrier, 2)

    ways = (
        (me, lax.rem(me + 1, n), me < n - 1, me > 0),
        (n - 1 - me, lax.rem(me + n - 1, n), me > 0, me < n - 1),
    )

    def span(k):
        return pl.ds(pl.multiple_of(k * rows, rows), rows)

    def copy(way, source, round_, k):
        return pltpu.make_async_remote_copy(
            src_ref=source,
            dst_ref=landed.at[way, round_, span(k)],
            send_sem=send_sem.at[way, round_, k],
            recv_sem=recv_sem.at[way, round_, k],
            device_id={"dp": ways[way][1]},
            device_id_type=MESH,
        )

    def start_own(way):
        @pl.when(ways[way][2])
        def _():
            @pl.loop(0, chunks)
            def _(k):
                copy(way, cot_ref.at[span(k)], 0, k).start()

    def column_tiles(body):
        @pl.loop(0, cols // tile)
        def _(c):
            body(pl.ds(pl.multiple_of(c * tile, tile), tile))

    def grad_of(read, block):
        total[...] = jnp.zeros_like(total)

        def add(at):
            total[...] += contract_last(read(at), masked_w[:, at])

        column_tiles(add)
        grad_ref[block] = total[...].astype(grad_ref.dtype)

    start_own(0)
    start_own(1)

    def query_tile(at):
        w = w_ref[:, at] * keep_ref[:, at]
        masked_w[:, at] = w
        product = jnp.dot(latent_ref[...], w, preferred_element_type=jnp.float32)
        parts[:, :, at] = product.astype(parts.dtype).reshape(n, count, tile)

    column_tiles(query_tile)
    grad_of(lambda at: cot_ref[:, at], me)

    for round_ in range(1, n):

        @pl.loop(0, chunks)
        def _(k):
            for way in (0, 1):
                place, _, has_next, has_prev = ways[way]
                at = span(k)

                @pl.when(has_prev)
                def _():
                    copy(way, landed.at[way, round_ - 1, at], round_ - 1, k).wait_recv()

                @pl.when(jnp.logical_and(has_next, place >= round_))
                def _():
                    copy(way, landed.at[way, round_ - 1, at], round_, k).start()

                @pl.when(jnp.logical_and(has_next, place < round_))
                def _():
                    ahead = place + n - round_
                    owner = ahead if way == 0 else n - 1 - ahead

                    @pl.when(has_prev)
                    def _():
                        def add(cs):
                            both = parts[owner, at, cs].astype(jnp.float32) + landed[
                                way, round_ - 1, at, cs
                            ].astype(jnp.float32)
                            parts[owner, at, cs] = both.astype(parts.dtype)

                        column_tiles(add)

                    copy(way, parts.at[owner, at], round_, k).start()

        for way in (0, 1):
            place = ways[way][0]

            @pl.when(place >= round_)
            def _():
                block = me - round_ if way == 0 else me + round_
                grad_of(lambda at: landed[way, round_ - 1, :, at], block)

    @pl.loop(0, chunks)
    def _(k):
        at = span(k)
        for way in (0, 1):

            @pl.when(ways[way][3])
            def _():
                copy(way, landed.at[way, n - 1, at], n - 1, k).wait_recv()

        def finish(used):
            def add(cs):
                value = parts[me, at, cs].astype(jnp.float32)
                for way in used:
                    value += landed[way, n - 1, at, cs].astype(jnp.float32)
                queries_ref[at, cs] = value.astype(queries_ref.dtype)

            column_tiles(add)

        pl.when(me == 0)(lambda: finish((1,)))
        pl.when(me == n - 1)(lambda: finish((0,)))
        pl.when(jnp.logical_and(me > 0, me < n - 1))(lambda: finish((0, 1)))

    for way in (0, 1):

        @pl.when(ways[way][2])
        def _():
            for round_ in range(n):

                @pl.loop(0, chunks)
                def _(k):
                    copy(way, landed.at[way, round_, span(k)], round_, k).wait_send()


def exchange(latent, w_up, keep, cotangent):
    n = lax.axis_size("dp")
    count, cols = cotangent.shape
    depth = w_up.shape[0]
    chunks = 4
    tile = 384 if cols % 384 == 0 else 128
    vmem = pl.BlockSpec(memory_space=pltpu.VMEM)
    bf16 = jnp.bfloat16
    return pl.pallas_call(
        functools.partial(exchange_kernel, n, chunks, tile),
        out_shape=(
            jax.ShapeDtypeStruct((count, cols), bf16),
            jax.ShapeDtypeStruct((n, count, depth), bf16),
        ),
        in_specs=[vmem] * 4,
        out_specs=(vmem, vmem),
        scratch_shapes=[
            pltpu.VMEM((depth, cols), bf16),
            pltpu.VMEM((n, count, cols), bf16),
            pltpu.VMEM((2, n, count, cols), bf16),
            pltpu.VMEM((count, depth), jnp.float32),
            pltpu.SemaphoreType.DMA((2, n, chunks)),
            pltpu.SemaphoreType.DMA((2, n, chunks)),
        ],
        compiler_params=pltpu.CompilerParams(
            collective_id=0, has_side_effects=True, vmem_limit_bytes=60 * 2**20
        ),
    )(latent, w_up, keep, cotangent)


def move_tokens_body(tokens, w_down, gain, w_up, head_counts, cotangent):
    n = lax.axis_size("mp")
    swap = [(i * n + j, j * n + i) for i in range(n) for j in range(n)]
    position = lax.axis_index("mp")
    latent_width = w_down.shape[1] * n
    keep_mask = keep_mask_of(head_counts, w_up.shape[1])

    def transpose_owner(block):
        return lax.ppermute(block, ("dp", "mp"), swap)

    rows = w_down.shape[0]
    tokens_block = lax.dynamic_slice_in_dim(tokens, position * rows, rows, 1)
    tokens_cols = lax.all_gather(transpose_owner(tokens_block), "mp", axis=0, tiled=True)
    raw_partial = jnp.dot(tokens_cols, w_down, preferred_element_type=jnp.float32)
    latent_raw = lax.psum_scatter(raw_partial, "dp", scatter_dimension=0, tiled=True)
    squares = lax.psum(jnp.sum(latent_raw * latent_raw, axis=1, keepdims=True), "mp")
    root_mean = jnp.sqrt(squares / latent_width + 1e-06)
    latent_local = (latent_raw / root_mean * gain).astype(jnp.bfloat16)
    latent = lax.all_gather(transpose_owner(latent_local), "mp", axis=0, tiled=True)
    keep_row = keep_mask.astype(jnp.bfloat16)[None, :]
    queries, grad_partial = exchange(latent, w_up, keep_row, cotangent)
    grad_partial = grad_partial.reshape(-1, grad_partial.shape[-1])
    grad_latent = transpose_owner(
        lax.psum_scatter(grad_partial, "mp", scatter_dimension=0, tiled=True)
    ).astype(jnp.float32)
    inner_dot = lax.psum(jnp.sum(gain * grad_latent * latent_raw, axis=1, keepdims=True), "mp")
    grad_raw = (
        gain * grad_latent / root_mean - latent_raw * inner_dot / (latent_width * root_mean**3)
    ).astype(jnp.bfloat16)
    grad_raw_all = lax.all_gather(grad_raw, "dp", axis=0, tiled=True)
    token_partial = contract_last(grad_raw_all, w_down).astype(jnp.bfloat16)
    grad_tokens = transpose_owner(
        lax.psum_scatter(token_partial, "mp", scatter_dimension=0, tiled=True)
    )
    return (queries, grad_tokens)


def solution(mesh):
    in_specs = (
        P(("groups", "dp"), None),
        P("dp", "mp"),
        P("mp"),
        P("dp", "mp"),
        P(),
        P(("groups", "dp"), "mp"),
    )
    out_specs = (P(("groups", "dp"), "mp"), P(("groups", "dp"), "mp"))
    square = mesh.shape["dp"] == mesh.shape["mp"]
    body = move_tokens_body if square else gather_weights_body
    return jax.shard_map(body, mesh=mesh, in_specs=in_specs, out_specs=out_specs, check_vma=False)
```

```python
import functools

import jax
import jax.numpy as jnp
from jax import lax
from jax.experimental import pallas as pl
from jax.experimental.pallas import tpu as pltpu
from jax.sharding import PartitionSpec as P

HD = 192
MESH = pl.DeviceIdType.MESH


def contract_last(left, right):
    return lax.dot_general(
        left, right, (((1,), (1,)), ((), ())), preferred_element_type=jnp.float32
    )


def keep_mask_of(head_counts, block_cols):
    position = lax.axis_index("mp")
    held_heads = lax.dynamic_slice_in_dim(head_counts, position, 1, 0)
    slot_index = jnp.arange(block_cols, dtype=jnp.int32) // HD
    return (slot_index < held_heads).astype(jnp.float32)


def gather_weights_body(tokens, w_down, gain, w_up, head_counts, cotangent):
    latent_width = w_down.shape[1] * lax.axis_size("mp")
    keep_mask = keep_mask_of(head_counts, w_up.shape[1])
    down_whole = lax.all_gather(w_down, "dp", axis=0, tiled=True)
    latent_raw = jnp.dot(tokens, down_whole, preferred_element_type=jnp.float32)
    squares = lax.psum(jnp.sum(latent_raw * latent_raw, axis=1, keepdims=True), "mp")
    root_mean = jnp.sqrt(squares / latent_width + 1e-06)
    latent_local = (latent_raw / root_mean * gain).astype(jnp.bfloat16)
    latent = lax.all_gather(latent_local, "mp", axis=1, tiled=True)
    masked = cotangent * keep_mask.astype(jnp.bfloat16)
    up_whole = lax.all_gather(w_up, "dp", axis=0, tiled=True)
    query_total = jnp.dot(latent, up_whole, preferred_element_type=jnp.float32)
    grad_partial = contract_last(masked, up_whole)
    queries = (query_total * keep_mask).astype(jnp.bfloat16)
    grad_latent = lax.psum_scatter(
        grad_partial.astype(jnp.bfloat16), "mp", scatter_dimension=1, tiled=True
    ).astype(jnp.float32)
    inner_dot = lax.psum(jnp.sum(gain * grad_latent * latent_raw, axis=1, keepdims=True), "mp")
    grad_raw = (
        gain * grad_latent / root_mean - latent_raw * inner_dot / (latent_width * root_mean**3)
    ).astype(jnp.bfloat16)
    partial_value = contract_last(grad_raw, down_whole).astype(jnp.bfloat16)
    grad_tokens = lax.psum_scatter(partial_value, "mp", scatter_dimension=1, tiled=True)
    return (queries, grad_tokens)


def exchange_kernel(
    n, chunks, tile, tokens_ref, down_ref, gain_ref, w_ref, keep_ref, cot_ref,
    queries_ref, grad_ref, raw_ref, root_ref,
    masked_w, parts, landed, total, send_sem, recv_sem,
    tokens_all, raw_total, raw_out, raw_in, square_out, square_in, latent_out, latent_all,
    small_send, small_recv,
):
    me = lax.axis_index("dp")
    count, cols = cot_ref.shape
    rows = count // chunks

    mine = lax.axis_index("mp")

    barrier = pltpu.get_barrier_semaphore()

    @pl.loop(0, n * n)
    def _(other):
        @pl.when(other != me * n + mine)
        def _():
            pl.semaphore_signal(
                barrier, inc=1,
                device_id={"dp": other // n, "mp": lax.rem(other, n)}, device_id_type=MESH,
            )

    pl.semaphore_wait(barrier, n * n - 1)

    def small(kind, slot, source, target, dp, mp):
        return pltpu.make_async_remote_copy(
            src_ref=source, dst_ref=target,
            send_sem=small_send.at[kind, slot], recv_sem=small_recv.at[kind, slot],
            device_id={"dp": dp, "mp": mp}, device_id_type=MESH,
        )

    ways = (
        (me, lax.rem(me + 1, n), me < n - 1, me > 0),
        (n - 1 - me, lax.rem(me + n - 1, n), me > 0, me < n - 1),
    )

    def span(k):
        return pl.ds(pl.multiple_of(k * rows, rows), rows)

    def copy(way, source, round_, k):
        return pltpu.make_async_remote_copy(
            src_ref=source,
            dst_ref=landed.at[way, round_, span(k)],
            send_sem=send_sem.at[way, round_, k],
            recv_sem=recv_sem.at[way, round_, k],
            device_id={"dp": ways[way][1]},
            device_id_type=MESH,
        )

    def start_own(way, first, last):
        @pl.when(ways[way][2])
        def _():
            @pl.loop(first, last)
            def _(k):
                copy(way, cot_ref.at[span(k)], 0, k).start()

    def column_tiles(body):
        @pl.loop(0, cols // tile)
        def _(c):
            body(pl.ds(pl.multiple_of(c * tile, tile), tile))

    def grad_of(read, block):
        total[...] = jnp.zeros_like(total)

        def add(at):
            total[...] += contract_last(read(at), masked_w[:, at])

        column_tiles(add)
        grad_ref[block] = total[...].astype(grad_ref.dtype)

    down_rows, width = down_ref.shape
    quarter = count // n
    far, near = lax.rem(mine + 2, n), mine + 1 - 2 * lax.rem(mine, 2)
    far_near = lax.rem(near + 2, n)

    def after(o):
        return lax.rem(me + o, n)

    def before(o):
        return lax.rem(me + n - o, n)

    def piece(block, who):
        return tokens_all.at[block, pl.ds(pl.multiple_of(who * quarter, quarter), quarter)]

    def token_columns(block):
        return pl.ds(pl.multiple_of(block * down_rows, down_rows), down_rows)

    started = []

    def go(c):
        c.start()
        started.append(c)

    for o in range(1, n):
        source = tokens_ref.at[
            pl.ds(pl.multiple_of(mine * quarter, quarter), quarter), token_columns(after(o))
        ]
        go(small(0, o, source, piece(me, mine), after(o), mine))
    for way in (0, 1):
        start_own(way, 0, chunks // 2)
    tokens_all[me] = tokens_ref[:, token_columns(me)]
    for o in range(1, n):
        block = before(o)
        held = piece(block, mine)
        small(0, o, held, held, me, far).wait_recv()
        go(small(1, o, held, held, me, far))
        go(small(2, o, held, held, me, near))
    for o in range(1, n):
        held = piece(before(o), far)
        small(1, o, held, held, me, far).wait_recv()
        go(small(3, o, held, held, me, near))
    for o in range(1, n):
        for kind, who in ((2, near), (3, far_near)):
            held = piece(before(o), who)
            small(kind, o, held, held, me, near).wait_recv()

    raw_total[...] = jnp.zeros_like(raw_total)
    depth_tile = 256 if down_rows % 256 == 0 else 128

    @pl.loop(0, down_rows // depth_tile)
    def _(c):
        at = pl.ds(pl.multiple_of(c * depth_tile, depth_tile), depth_tile)
        raw_total[...] += jnp.dot(
            tokens_all[:, :, at].reshape(n * count, depth_tile), down_ref[at, :],
            preferred_element_type=jnp.float32,
        )

    raw_out[...] = raw_total[...].astype(raw_out.dtype).reshape(raw_out.shape)
    for o in range(1, n):
        go(small(4, o, raw_out.at[after(o)], raw_in.at[o - 1], after(o), mine))
    for way in (0, 1):
        start_own(way, chunks // 2, chunks)
    raw = raw_total[pl.ds(pl.multiple_of(me * count, count), count), :]
    for o in range(1, n):
        small(4, o, raw_out.at[me], raw_in.at[o - 1], after(o), mine).wait_recv()
        raw += raw_in[o - 1].astype(jnp.float32)
    raw_ref[...] = raw
    square_out[...] = jnp.broadcast_to(
        jnp.sum(raw * raw, axis=1, keepdims=True), square_out.shape
    )
    for o in range(1, n):
        go(small(5, o, square_out, square_in.at[o - 1], me, lax.rem(mine + o, n)))
    squares = square_out[...]
    for o in range(1, n):
        small(5, o, square_out, square_in.at[o - 1], me, mine).wait_recv()
        squares += square_in[o - 1]
    root = jnp.sqrt(squares / (width * n) + 1e-06)
    root_ref[...] = root
    latent_out[...] = (raw_ref[...] / root[:, :1] * gain_ref[...]).astype(latent_out.dtype)

    on_diagonal = me == mine

    def latent_slot(block):
        return latent_all.at[pl.ds(pl.multiple_of(block * count, count), count)]

    def latent_copy(to):
        return pltpu.make_async_remote_copy(
            src_ref=latent_out, dst_ref=latent_slot(me),
            send_sem=small_send.at[6, to], recv_sem=small_recv.at[6, me],
            device_id={"dp": mine, "mp": to}, device_id_type=MESH,
        )

    for to in range(n):
        itself = jnp.logical_and(on_diagonal, mine == to)
        pl.when(jnp.logical_not(itself))(lambda to=to: latent_copy(to).start())

    @pl.when(on_diagonal)
    def _():
        latent_all[pl.ds(pl.multiple_of(me * count, count), count), :] = latent_out[...]

    for block in range(n):
        itself = jnp.logical_and(on_diagonal, me == block)

        @pl.when(jnp.logical_not(itself))
        def _():
            small(6, block, latent_out, latent_slot(block), me, near).wait_recv()

    def query_tile(at):
        w = w_ref[:, at] * keep_ref[:, at]
        masked_w[:, at] = w
        product = jnp.dot(latent_all[...], w, preferred_element_type=jnp.float32)
        parts[:, :, at] = product.astype(parts.dtype).reshape(n, count, tile)

    column_tiles(query_tile)
    grad_of(lambda at: cot_ref[:, at], me)

    for round_ in range(1, n):

        @pl.loop(0, chunks)
        def _(k):
            for way in (0, 1):
                place, _, has_next, has_prev = ways[way]
                at = span(k)

                @pl.when(has_prev)
                def _():
                    copy(way, landed.at[way, round_ - 1, at], round_ - 1, k).wait_recv()

                @pl.when(jnp.logical_and(has_next, place >= round_))
                def _():
                    copy(way, landed.at[way, round_ - 1, at], round_, k).start()

                @pl.when(jnp.logical_and(has_next, place < round_))
                def _():
                    ahead = place + n - round_
                    owner = ahead if way == 0 else n - 1 - ahead

                    @pl.when(has_prev)
                    def _():
                        def add(cs):
                            both = parts[owner, at, cs].astype(jnp.float32) + landed[
                                way, round_ - 1, at, cs
                            ].astype(jnp.float32)
                            parts[owner, at, cs] = both.astype(parts.dtype)

                        column_tiles(add)

                    copy(way, parts.at[owner, at], round_, k).start()

        for way in (0, 1):
            place = ways[way][0]

            @pl.when(place >= round_)
            def _():
                block = me - round_ if way == 0 else me + round_
                grad_of(lambda at: landed[way, round_ - 1, :, at], block)

    @pl.loop(0, chunks)
    def _(k):
        at = span(k)
        for way in (0, 1):

            @pl.when(ways[way][3])
            def _():
                copy(way, landed.at[way, n - 1, at], n - 1, k).wait_recv()

        def finish(used):
            def add(cs):
                value = parts[me, at, cs].astype(jnp.float32)
                for way in used:
                    value += landed[way, n - 1, at, cs].astype(jnp.float32)
                queries_ref[at, cs] = value.astype(queries_ref.dtype)

            column_tiles(add)

        pl.when(me == 0)(lambda: finish((1,)))
        pl.when(me == n - 1)(lambda: finish((0,)))
        pl.when(jnp.logical_and(me > 0, me < n - 1))(lambda: finish((0, 1)))

    for way in (0, 1):

        @pl.when(ways[way][2])
        def _():
            for round_ in range(n):

                @pl.loop(0, chunks)
                def _(k):
                    copy(way, landed.at[way, round_, span(k)], round_, k).wait_send()

    for c in started:
        c.wait_send()
    for to in range(n):
        itself = jnp.logical_and(on_diagonal, mine == to)
        pl.when(jnp.logical_not(itself))(lambda to=to: latent_copy(to).wait_send())


def exchange(tokens, w_down, gain, w_up, keep, cotangent):
    n = lax.axis_size("dp")
    count, cols = cotangent.shape
    depth = w_up.shape[0]
    chunks = 4
    tile = 384 if cols % 384 == 0 else 128
    vmem = pl.BlockSpec(memory_space=pltpu.VMEM)
    bf16 = jnp.bfloat16
    return pl.pallas_call(
        functools.partial(exchange_kernel, n, chunks, tile),
        out_shape=(
            jax.ShapeDtypeStruct((count, cols), bf16),
            jax.ShapeDtypeStruct((n, count, depth), bf16),
            jax.ShapeDtypeStruct((count, depth), jnp.float32),
            jax.ShapeDtypeStruct((count, 128), jnp.float32),
        ),
        in_specs=[vmem] * 6,
        out_specs=(vmem,) * 4,
        scratch_shapes=[
            pltpu.VMEM((depth, cols), bf16),
            pltpu.VMEM((n, count, cols), bf16),
            pltpu.VMEM((2, n, count, cols), bf16),
            pltpu.VMEM((count, depth), jnp.float32),
            pltpu.SemaphoreType.DMA((2, n, chunks)),
            pltpu.SemaphoreType.DMA((2, n, chunks)),
            pltpu.VMEM((n, count, w_down.shape[0]), bf16),
            pltpu.VMEM((n * count, depth), jnp.float32),
            pltpu.VMEM((n, count, depth), bf16),
            pltpu.VMEM((n - 1, count, depth), bf16),
            pltpu.VMEM((count, 128), jnp.float32),
            pltpu.VMEM((n - 1, count, 128), jnp.float32),
            pltpu.VMEM((count, depth), bf16),
            pltpu.VMEM((n * count, depth), bf16),
            pltpu.SemaphoreType.DMA((7, n)),
            pltpu.SemaphoreType.DMA((7, n)),
        ],
        compiler_params=pltpu.CompilerParams(
            collective_id=0, has_side_effects=True, vmem_limit_bytes=60 * 2**20
        ),
    )(tokens, w_down, gain, w_up, keep, cotangent)


def move_tokens_body(tokens, w_down, gain, w_up, head_counts, cotangent):
    n = lax.axis_size("mp")
    swap = [(i * n + j, j * n + i) for i in range(n) for j in range(n)]
    latent_width = w_down.shape[1] * n
    keep_mask = keep_mask_of(head_counts, w_up.shape[1])

    def transpose_owner(block):
        return lax.ppermute(block, ("dp", "mp"), swap)

    keep_row = keep_mask.astype(jnp.bfloat16)[None, :]
    queries, grad_partial, latent_raw, root_mean = exchange(
        tokens, w_down, gain[None, :], w_up, keep_row, cotangent
    )
    root_mean = root_mean[:, :1]
    grad_partial = grad_partial.reshape(-1, grad_partial.shape[-1])
    grad_latent = transpose_owner(
        lax.psum_scatter(grad_partial, "mp", scatter_dimension=0, tiled=True)
    ).astype(jnp.float32)
    inner_dot = lax.psum(jnp.sum(gain * grad_latent * latent_raw, axis=1, keepdims=True), "mp")
    grad_raw = (
        gain * grad_latent / root_mean - latent_raw * inner_dot / (latent_width * root_mean**3)
    ).astype(jnp.bfloat16)
    grad_raw_all = lax.all_gather(grad_raw, "dp", axis=0, tiled=True)
    token_partial = contract_last(grad_raw_all, w_down).astype(jnp.bfloat16)
    grad_tokens = transpose_owner(
        lax.psum_scatter(token_partial, "mp", scatter_dimension=0, tiled=True)
    )
    return (queries, grad_tokens)


def solution(mesh):
    in_specs = (
        P(("groups", "dp"), None),
        P("dp", "mp"),
        P("mp"),
        P("dp", "mp"),
        P(),
        P(("groups", "dp"), "mp"),
    )
    out_specs = (P(("groups", "dp"), "mp"), P(("groups", "dp"), "mp"))
    square = mesh.shape["dp"] == mesh.shape["mp"] == 4
    body = move_tokens_body if square else gather_weights_body
    return jax.shard_map(body, mesh=mesh, in_specs=in_specs, out_specs=out_specs, check_vma=False)
```

```python
import functools

import jax
import jax.numpy as jnp
from jax import lax
from jax.experimental import pallas as pl
from jax.experimental.pallas import tpu as pltpu
from jax.sharding import PartitionSpec as P

HD = 192
MESH = pl.DeviceIdType.MESH


def contract_last(left, right):
    return lax.dot_general(
        left, right, (((1,), (1,)), ((), ())), preferred_element_type=jnp.float32
    )


def keep_mask_of(head_counts, block_cols):
    position = lax.axis_index("mp")
    held_heads = lax.dynamic_slice_in_dim(head_counts, position, 1, 0)
    slot_index = jnp.arange(block_cols, dtype=jnp.int32) // HD
    return (slot_index < held_heads).astype(jnp.float32)


def gather_weights_body(tokens, w_down, gain, w_up, head_counts, cotangent):
    latent_width = w_down.shape[1] * lax.axis_size("mp")
    keep_mask = keep_mask_of(head_counts, w_up.shape[1])
    down_whole = lax.all_gather(w_down, "dp", axis=0, tiled=True)
    latent_raw = jnp.dot(tokens, down_whole, preferred_element_type=jnp.float32)
    squares = lax.psum(jnp.sum(latent_raw * latent_raw, axis=1, keepdims=True), "mp")
    root_mean = jnp.sqrt(squares / latent_width + 1e-06)
    latent_local = (latent_raw / root_mean * gain).astype(jnp.bfloat16)
    latent = lax.all_gather(latent_local, "mp", axis=1, tiled=True)
    masked = cotangent * keep_mask.astype(jnp.bfloat16)
    up_whole = lax.all_gather(w_up, "dp", axis=0, tiled=True)
    query_total = jnp.dot(latent, up_whole, preferred_element_type=jnp.float32)
    grad_partial = contract_last(masked, up_whole)
    queries = (query_total * keep_mask).astype(jnp.bfloat16)
    grad_latent = lax.psum_scatter(
        grad_partial.astype(jnp.bfloat16), "mp", scatter_dimension=1, tiled=True
    ).astype(jnp.float32)
    inner_dot = lax.psum(jnp.sum(gain * grad_latent * latent_raw, axis=1, keepdims=True), "mp")
    grad_raw = (
        gain * grad_latent / root_mean - latent_raw * inner_dot / (latent_width * root_mean**3)
    ).astype(jnp.bfloat16)
    partial_value = contract_last(grad_raw, down_whole).astype(jnp.bfloat16)
    grad_tokens = lax.psum_scatter(partial_value, "mp", scatter_dimension=1, tiled=True)
    return (queries, grad_tokens)


def exchange_kernel(
    n, chunks, tile, tokens_ref, down_ref, gain_ref, w_ref, keep_ref, cot_ref,
    queries_ref, grad_tokens_ref, raw_ref, root_ref, grad_ref, grad_in, grad_all,
    products, near_in, far_in, pair_out, block_out, block_in, dot_out, dot_in,
    masked_w, parts, landed, total, send_sem, recv_sem,
    tokens_all, raw_total, raw_out, raw_in, square_out, square_in, latent_out, latent_all,
    small_send, small_recv,
):
    me = lax.axis_index("dp")
    count, cols = cot_ref.shape
    rows = count // chunks

    mine = lax.axis_index("mp")

    barrier = pltpu.get_barrier_semaphore()

    @pl.loop(0, n * n)
    def _(other):
        @pl.when(other != me * n + mine)
        def _():
            pl.semaphore_signal(
                barrier, inc=1,
                device_id={"dp": other // n, "mp": lax.rem(other, n)}, device_id_type=MESH,
            )

    pl.semaphore_wait(barrier, n * n - 1)

    def small(kind, slot, source, target, dp, mp):
        return pltpu.make_async_remote_copy(
            src_ref=source, dst_ref=target,
            send_sem=small_send.at[kind, slot], recv_sem=small_recv.at[kind, slot],
            device_id={"dp": dp, "mp": mp}, device_id_type=MESH,
        )

    ways = (
        (me, lax.rem(me + 1, n), me < n - 1, me > 0),
        (n - 1 - me, lax.rem(me + n - 1, n), me > 0, me < n - 1),
    )

    def span(k):
        return pl.ds(pl.multiple_of(k * rows, rows), rows)

    def copy(way, source, round_, k):
        return pltpu.make_async_remote_copy(
            src_ref=source,
            dst_ref=landed.at[way, round_, span(k)],
            send_sem=send_sem.at[way, round_, k],
            recv_sem=recv_sem.at[way, round_, k],
            device_id={"dp": ways[way][1]},
            device_id_type=MESH,
        )

    def start_own(way, first, last):
        @pl.when(ways[way][2])
        def _():
            @pl.loop(first, last)
            def _(k):
                copy(way, cot_ref.at[span(k)], 0, k).start()

    def column_tiles(body):
        @pl.loop(0, cols // tile)
        def _(c):
            body(pl.ds(pl.multiple_of(c * tile, tile), tile))

    def grad_of(read, block):
        total[...] = jnp.zeros_like(total)

        def add(at):
            total[...] += contract_last(read(at), masked_w[:, at])

        column_tiles(add)
        grad_ref[block] = total[...].astype(grad_ref.dtype)
        itself = jnp.logical_and(on_diagonal, block == me)

        @pl.when(jnp.logical_not(itself))
        def _():
            grad_copy(block).start()

        @pl.when(itself)
        def _():
            grad_in[mine] = grad_ref[block]

    def grad_copy(block):
        return pltpu.make_async_remote_copy(
            src_ref=grad_ref.at[block], dst_ref=grad_in.at[mine],
            send_sem=small_send.at[7, block], recv_sem=small_recv.at[7, mine],
            device_id={"dp": block, "mp": me}, device_id_type=MESH,
        )

    down_rows, width = down_ref.shape
    quarter = count // n
    far, near = lax.rem(mine + 2, n), mine + 1 - 2 * lax.rem(mine, 2)
    far_near = lax.rem(near + 2, n)

    def after(o):
        return lax.rem(me + o, n)

    def before(o):
        return lax.rem(me + n - o, n)

    def piece(block, who):
        return tokens_all.at[block, pl.ds(pl.multiple_of(who * quarter, quarter), quarter)]

    def token_columns(block):
        return pl.ds(pl.multiple_of(block * down_rows, down_rows), down_rows)

    started = []

    def go(c):
        c.start()
        started.append(c)

    for o in range(1, n):
        source = tokens_ref.at[
            pl.ds(pl.multiple_of(mine * quarter, quarter), quarter), token_columns(after(o))
        ]
        go(small(0, o, source, piece(me, mine), after(o), mine))
    for way in (0, 1):
        start_own(way, 0, chunks // 2)
    tokens_all[me] = tokens_ref[:, token_columns(me)]
    for o in range(1, n):
        block = before(o)
        held = piece(block, mine)
        small(0, o, held, held, me, far).wait_recv()
        go(small(1, o, held, held, me, far))
        go(small(2, o, held, held, me, near))
    for o in range(1, n):
        held = piece(before(o), far)
        small(1, o, held, held, me, far).wait_recv()
        go(small(3, o, held, held, me, near))
    for o in range(1, n):
        for kind, who in ((2, near), (3, far_near)):
            held = piece(before(o), who)
            small(kind, o, held, held, me, near).wait_recv()

    raw_total[...] = jnp.zeros_like(raw_total)
    depth_tile = 256 if down_rows % 256 == 0 else 128

    @pl.loop(0, down_rows // depth_tile)
    def _(c):
        at = pl.ds(pl.multiple_of(c * depth_tile, depth_tile), depth_tile)
        raw_total[...] += jnp.dot(
            tokens_all[:, :, at].reshape(n * count, depth_tile), down_ref[at, :],
            preferred_element_type=jnp.float32,
        )

    raw_out[...] = raw_total[...].astype(raw_out.dtype).reshape(raw_out.shape)
    for o in range(1, n):
        go(small(4, o, raw_out.at[after(o)], raw_in.at[o - 1], after(o), mine))
    for way in (0, 1):
        start_own(way, chunks // 2, chunks)
    raw = raw_total[pl.ds(pl.multiple_of(me * count, count), count), :]
    for o in range(1, n):
        small(4, o, raw_out.at[me], raw_in.at[o - 1], after(o), mine).wait_recv()
        raw += raw_in[o - 1].astype(jnp.float32)
    raw_ref[...] = raw
    square_out[...] = jnp.broadcast_to(
        jnp.sum(raw * raw, axis=1, keepdims=True), square_out.shape
    )
    for o in range(1, n):
        go(small(5, o, square_out, square_in.at[o - 1], me, lax.rem(mine + o, n)))
    squares = square_out[...]
    for o in range(1, n):
        small(5, o, square_out, square_in.at[o - 1], me, mine).wait_recv()
        squares += square_in[o - 1]
    root = jnp.sqrt(squares / (width * n) + 1e-06)
    root_ref[...] = root
    latent_out[...] = (raw_ref[...] / root[:, :1] * gain_ref[...]).astype(latent_out.dtype)

    on_diagonal = me == mine

    def latent_slot(block):
        return latent_all.at[pl.ds(pl.multiple_of(block * count, count), count)]

    def latent_copy(to):
        return pltpu.make_async_remote_copy(
            src_ref=latent_out, dst_ref=latent_slot(me),
            send_sem=small_send.at[6, to], recv_sem=small_recv.at[6, me],
            device_id={"dp": mine, "mp": to}, device_id_type=MESH,
        )

    for to in range(n):
        itself = jnp.logical_and(on_diagonal, mine == to)
        pl.when(jnp.logical_not(itself))(lambda to=to: latent_copy(to).start())

    @pl.when(on_diagonal)
    def _():
        latent_all[pl.ds(pl.multiple_of(me * count, count), count), :] = latent_out[...]

    for block in range(n):
        itself = jnp.logical_and(on_diagonal, me == block)

        @pl.when(jnp.logical_not(itself))
        def _():
            small(6, block, latent_out, latent_slot(block), me, near).wait_recv()

    def query_tile(at):
        w = w_ref[:, at] * keep_ref[:, at]
        masked_w[:, at] = w
        product = jnp.dot(latent_all[...], w, preferred_element_type=jnp.float32)
        parts[:, :, at] = product.astype(parts.dtype).reshape(n, count, tile)

    column_tiles(query_tile)
    grad_of(lambda at: cot_ref[:, at], me)

    for round_ in range(1, n):

        @pl.loop(0, chunks)
        def _(k):
            for way in (0, 1):
                place, _, has_next, has_prev = ways[way]
                at = span(k)

                @pl.when(has_prev)
                def _():
                    copy(way, landed.at[way, round_ - 1, at], round_ - 1, k).wait_recv()

                @pl.when(jnp.logical_and(has_next, place >= round_))
                def _():
                    copy(way, landed.at[way, round_ - 1, at], round_, k).start()

                @pl.when(jnp.logical_and(has_next, place < round_))
                def _():
                    ahead = place + n - round_
                    owner = ahead if way == 0 else n - 1 - ahead

                    @pl.when(has_prev)
                    def _():
                        def add(cs):
                            both = parts[owner, at, cs].astype(jnp.float32) + landed[
                                way, round_ - 1, at, cs
                            ].astype(jnp.float32)
                            parts[owner, at, cs] = both.astype(parts.dtype)

                        column_tiles(add)

                    copy(way, parts.at[owner, at], round_, k).start()

        for way in (0, 1):
            place = ways[way][0]

            @pl.when(place >= round_)
            def _():
                block = me - round_ if way == 0 else me + round_
                grad_of(lambda at: landed[way, round_ - 1, :, at], block)

    for who in range(n):
        itself = jnp.logical_and(on_diagonal, mine == who)

        @pl.when(jnp.logical_not(itself))
        def _():
            small(7, who, grad_ref.at[0], grad_in.at[who], me, near).wait_recv()

    grad_latent = grad_in[0].astype(jnp.float32)
    for who in range(1, n):
        grad_latent += grad_in[who].astype(jnp.float32)
    scaled = gain_ref[...] * grad_latent
    raw = raw_ref[...]
    dot_out[...] = jnp.broadcast_to(
        jnp.sum(scaled * raw, axis=1, keepdims=True), dot_out.shape
    )
    for o in range(1, n):
        go(small(8, o, dot_out, dot_in.at[o - 1], me, lax.rem(mine + o, n)))
    inner = dot_out[...]
    for o in range(1, n):
        small(8, o, dot_out, dot_in.at[o - 1], me, mine).wait_recv()
        inner += dot_in[o - 1]
    root = root_ref[...]
    slope = (inner / (width * n * (root * root * root)))[:, :1]
    grad_all[me] = (scaled / root[:, :1] - raw * slope).astype(grad_all.dtype)
    for o in range(1, n):
        go(small(9, o, grad_all.at[me], grad_all.at[me], after(o), mine))

    @pl.loop(0, chunks)
    def _(k):
        at = span(k)
        for way in (0, 1):

            @pl.when(ways[way][3])
            def _():
                copy(way, landed.at[way, n - 1, at], n - 1, k).wait_recv()

        def finish(used):
            def add(cs):
                value = parts[me, at, cs].astype(jnp.float32)
                for way in used:
                    value += landed[way, n - 1, at, cs].astype(jnp.float32)
                queries_ref[at, cs] = value.astype(queries_ref.dtype)

            column_tiles(add)

        pl.when(me == 0)(lambda: finish((1,)))
        pl.when(me == n - 1)(lambda: finish((0,)))
        pl.when(jnp.logical_and(me > 0, me < n - 1))(lambda: finish((0, 1)))

    for o in range(1, n):
        held = grad_all.at[before(o)]
        small(9, o, held, held, after(o), mine).wait_recv()

    def row_tiles(body):
        @pl.loop(0, down_rows // depth_tile)
        def _(c):
            body(pl.ds(pl.multiple_of(c * depth_tile, depth_tile), depth_tile))

    def product_tile(at):
        product = contract_last(grad_all[...].reshape(n * count, width), down_ref[at, :])
        products[:, :, at] = product.astype(products.dtype).reshape(n, count, depth_tile)

    row_tiles(product_tile)
    go(small(10, 0, products.at[far_near], near_in.at[1], me, near))
    go(small(10, 1, products.at[near], near_in.at[0], me, near))
    small(10, 0, products.at[far_near], near_in.at[1], me, near).wait_recv()

    def pair_tile(at):
        both = products[far, :, at].astype(jnp.float32) + near_in[1, :, at].astype(jnp.float32)
        pair_out[:, at] = both.astype(pair_out.dtype)

    row_tiles(pair_tile)
    go(small(11, 0, pair_out, far_in, me, far))
    small(10, 1, products.at[near], near_in.at[0], me, near).wait_recv()
    small(11, 0, pair_out, far_in, me, far).wait_recv()

    def sum_tile(at):
        both = products[mine, :, at].astype(jnp.float32) + near_in[0, :, at].astype(jnp.float32)
        block_out[:, at] = (both + far_in[:, at].astype(jnp.float32)).astype(block_out.dtype)

    row_tiles(sum_tile)
    last = small(12, 0, block_out, block_in, mine, me)

    @pl.when(jnp.logical_not(on_diagonal))
    def _():
        last.start()
        last.wait()
        grad_tokens_ref[...] = block_in[...]

    @pl.when(on_diagonal)
    def _():
        grad_tokens_ref[...] = block_out[...]

    for block in range(n):
        itself = jnp.logical_and(on_diagonal, me == block)
        pl.when(jnp.logical_not(itself))(lambda block=block: grad_copy(block).wait_send())

    for way in (0, 1):

        @pl.when(ways[way][2])
        def _():
            for round_ in range(n):

                @pl.loop(0, chunks)
                def _(k):
                    copy(way, landed.at[way, round_, span(k)], round_, k).wait_send()

    for c in started:
        c.wait_send()
    for to in range(n):
        itself = jnp.logical_and(on_diagonal, mine == to)
        pl.when(jnp.logical_not(itself))(lambda to=to: latent_copy(to).wait_send())


def exchange(tokens, w_down, gain, w_up, keep, cotangent):
    n = lax.axis_size("dp")
    count, cols = cotangent.shape
    depth = w_up.shape[0]
    down_rows = w_down.shape[0]
    chunks = 4
    tile = 384 if cols % 384 == 0 else 128
    vmem = pl.BlockSpec(memory_space=pltpu.VMEM)
    bf16 = jnp.bfloat16
    return pl.pallas_call(
        functools.partial(exchange_kernel, n, chunks, tile),
        out_shape=(
            jax.ShapeDtypeStruct((count, cols), bf16),
            jax.ShapeDtypeStruct((count, down_rows), bf16),
        ),
        in_specs=[vmem] * 6,
        out_specs=(vmem,) * 2,
        scratch_shapes=[
            pltpu.VMEM((count, depth), jnp.float32),
            pltpu.VMEM((count, 128), jnp.float32),
            pltpu.VMEM((n, count, depth), bf16),
            pltpu.VMEM((n, count, depth), bf16),
            pltpu.VMEM((n, count, depth), bf16),
            pltpu.VMEM((n, count, down_rows), bf16),
            pltpu.VMEM((2, count, down_rows), bf16),
            pltpu.VMEM((count, down_rows), bf16),
            pltpu.VMEM((count, down_rows), bf16),
            pltpu.VMEM((count, down_rows), bf16),
            pltpu.VMEM((count, down_rows), bf16),
            pltpu.VMEM((count, 128), jnp.float32),
            pltpu.VMEM((n - 1, count, 128), jnp.float32),
            pltpu.VMEM((depth, cols), bf16),
            pltpu.VMEM((n, count, cols), bf16),
            pltpu.VMEM((2, n, count, cols), bf16),
            pltpu.VMEM((count, depth), jnp.float32),
            pltpu.SemaphoreType.DMA((2, n, chunks)),
            pltpu.SemaphoreType.DMA((2, n, chunks)),
            pltpu.VMEM((n, count, w_down.shape[0]), bf16),
            pltpu.VMEM((n * count, depth), jnp.float32),
            pltpu.VMEM((n, count, depth), bf16),
            pltpu.VMEM((n - 1, count, depth), bf16),
            pltpu.VMEM((count, 128), jnp.float32),
            pltpu.VMEM((n - 1, count, 128), jnp.float32),
            pltpu.VMEM((count, depth), bf16),
            pltpu.VMEM((n * count, depth), bf16),
            pltpu.SemaphoreType.DMA((13, n)),
            pltpu.SemaphoreType.DMA((13, n)),
        ],
        compiler_params=pltpu.CompilerParams(
            collective_id=0, has_side_effects=True, vmem_limit_bytes=60 * 2**20
        ),
    )(tokens, w_down, gain, w_up, keep, cotangent)


def move_tokens_body(tokens, w_down, gain, w_up, head_counts, cotangent):
    keep_row = keep_mask_of(head_counts, w_up.shape[1]).astype(jnp.bfloat16)[None, :]
    return exchange(tokens, w_down, gain[None, :], w_up, keep_row, cotangent)


def solution(mesh):
    in_specs = (
        P(("groups", "dp"), None),
        P("dp", "mp"),
        P("mp"),
        P("dp", "mp"),
        P(),
        P(("groups", "dp"), "mp"),
    )
    out_specs = (P(("groups", "dp"), "mp"), P(("groups", "dp"), "mp"))
    square = mesh.shape["dp"] == mesh.shape["mp"] == 4
    body = move_tokens_body if square else gather_weights_body
    return jax.shard_map(body, mesh=mesh, in_specs=in_specs, out_specs=out_specs, check_vma=False)
```
